32 devices in a mesh: groups: 2 (over y), row: 16 (over z, x, core).
Axes of the slice: x: 2, y: 2, z: 4, core: 2. Of those that a mesh axis runs over, the one named last changes fastest.
Arguments:
- walkers: bfloat16 [64, 1024, 256], P('groups', 'row'), parts along dimension 0, may hold values from -6 to 6
- cholesky: bfloat16 [1024, 1024, 1024], P('groups', 'row'), parts along dimension 0, may hold values from -0.03125 to 0.03125
- slab_index: int32 [4, 64], P('groups'), parts along dimension 0, may hold values from 0 to 511
- fields: bfloat16 [2, 64, 64], P(None, ('groups', 'row')), parts along dimension 1, may hold values from -5 to 5
- counts: int32 [32], P('groups'), parts along dimension 0, may hold values from 1 to 2, as said below
- sources: int32 [4, 32], P('groups'), parts along dimension 0, may hold values from 0 to 31, as said below
Outputs:
- branched: bfloat16 [64, 1024, 256], P('groups', 'row'), parts along dimension 0
The draws below stay inside these ranges and needn't reach their ends.
There are 2 independent parts, one for each index of `groups`. The reference program is written for one: setup_inputs(seed, part) draws one part's arguments, and reference() takes and returns one part's arrays. A program takes and returns all parts, laid end to end along the dimension named above; each array names one. Nothing has to cross between parts.
Inputs may be any that keep to these rules, and one draw needn't show every extreme that they name: counts[d] walkers live in the first counts[d] of the 2 slots d * 2 ... ; some index has all 2 live. For a living slot j, sources[s, j] is a living slot; for any other slot it is j itself.
All inputs are finite; a program needn't handle non-finite values.
Results may differ from the reference program's by a relative error of at most 0.0086.
Values may be sent and summed in bfloat16 or wider, within the bound.
A program may use at most 192 MiB of HBM per device.

```python
import jax
import jax.numpy as jnp
from jax import lax

NORB = 1024
NEL = 256
SLAB = 64
POOL = 512
WALK_DEV = 2
STEPS = 2
NW = 32
N_ROW = 16


def walker_counts(key):
    levels = jax.random.randint(jax.random.fold_in(key, 11), (N_ROW,), 0, 10)
    counted = 1 + levels * levels * (WALK_DEV - 1) // 81
    fullest = jax.random.randint(jax.random.fold_in(key, 12), (), 0, N_ROW)
    offset = jax.random.randint(jax.random.fold_in(key, 13), (), 1, N_ROW)
    counted = counted.at[fullest].set(WALK_DEV)
    counted = counted.at[(fullest + offset) % N_ROW].set(1)
    return counted.astype(jnp.int32)


def draw_counts(key, part):
    return walker_counts(key)


def draw_sources(key, part):
    counted = walker_counts(key)
    slot_count = WALK_DEV * N_ROW
    slot_ids = jnp.arange(slot_count, dtype=jnp.int32)
    inclusive = jnp.cumsum(counted)
    before = inclusive - counted
    live_total = inclusive[-1]
    ranks = jax.random.randint(jax.random.fold_in(key, 14), (STEPS, slot_count), 0, live_total)
    owners = jnp.sum((inclusive[None, None, :] <= ranks[:, :, None]).astype(jnp.int32), axis=2)
    picked = owners * WALK_DEV + ranks - jnp.take(before, owners)
    living = slot_ids % WALK_DEV < jnp.take(counted, slot_ids // WALK_DEV)
    return jnp.where(living[None, :], picked, slot_ids[None, :]).astype(jnp.int32)


def place_ends(result, key, least, largest):
    dims = result.shape
    place = [jax.random.randint(jax.random.fold_in(key, axis), (), 0, dims[axis]) for axis in range(len(dims))]
    result = result.at[tuple(place)].set(least)
    longest = dims.index(max(dims))
    place[longest] = (place[longest] + 1) % dims[longest]
    return result.at[tuple(place)].set(largest)


def shard_levels(own_key, dims, shards, least, largest):
    level, own = 1.0, jax.random.fold_in(own_key, 6)
    for position, shards_of in shards:
        draws = jnp.exp(jax.random.uniform(jax.random.fold_in(own, position), (shards_of,), jnp.float32, least / len(shards), largest / len(shards)))
        level = level * jnp.repeat(draws, dims[position] // shards_of).reshape([-1 if axis == position else 1 for axis in range(len(dims))])
    return level


def normal_values(own_key, shape, deviation, bound, pieces=(), held_as=jnp.bfloat16):
    loudness = shard_levels(own_key, shape, pieces, -0.22, 0.18) if pieces else 1.0
    array = jax.random.normal(own_key, shape, jnp.float32) * deviation * loudness
    return jnp.minimum(jnp.maximum(array, -bound), bound).astype(held_as)


def setup_inputs(seed: int = 0, part: int = 0) -> dict:
    keys = jax.random.split(jax.random.key(seed), 7)
    part_splits = jax.random.split(jax.random.fold_in(keys[6], part), 7)
    walkers = normal_values(part_splits[0], (NW, NORB, NEL), 1.0, 6.0, ((1, 16),))
    cholesky = normal_values(part_splits[1], (POOL, NORB, NORB), (NORB * SLAB // 2) ** -0.5, 0.03125, ((1, 16),))
    slab_index = place_ends(jax.random.randint(part_splits[2], (STEPS, SLAB), 0, POOL), jax.random.fold_in(part_splits[2], 1), 0, POOL - 1).astype(jnp.int32)
    fields = normal_values(part_splits[3], (STEPS, NW, SLAB), 1.0, 5.0, ((1, 16),))
    counts = draw_counts(jax.random.fold_in(jax.random.fold_in(keys[6], part), 71), part)
    sources = draw_sources(jax.random.fold_in(jax.random.fold_in(keys[6], part), 71), part)
    return {"walkers": walkers, "cholesky": cholesky, "slab_index": slab_index, "fields": fields, "counts": counts, "sources": sources}


def taylor_step(potential, initial):
    summed = initial.astype(jnp.float32)
    term_now = initial
    for degree in range(1, 5):
        product = jnp.dot(potential, term_now, preferred_element_type=jnp.float32) / degree
        summed = summed + product
        term_now = product.astype(jnp.bfloat16)
    return summed.astype(jnp.bfloat16)


def reference(walkers, cholesky, slab_index, fields, counts, sources):
    slot_count = walkers.shape[0]
    per_device = slot_count // N_ROW
    block_size = per_device * 8
    slot_ids = jnp.arange(slot_count, dtype=jnp.int32)
    living = (slot_ids % per_device) < jnp.take(counts, slot_ids // per_device)
    current = walkers
    for step_number in range(STEPS):
        chosen = jnp.take(cholesky, slab_index[step_number], axis=0).reshape(SLAB, NORB * NORB)

        def one_block(packed):
            block_fields, block_walkers, block_living = packed
            joined = jnp.dot(block_fields, chosen, preferred_element_type=jnp.float32)
            potentials = lax.optimization_barrier(joined.astype(jnp.bfloat16)).reshape(block_size, NORB, NORB)

            def one_walker(inner):
                matrix, initial, is_live = inner
                return lax.cond(is_live, lambda pair: taylor_step(pair[0], pair[1]), lambda pair: jnp.zeros_like(pair[1]), (matrix, initial))

            return lax.map(one_walker, (potentials, block_walkers, block_living))

        propagated = lax.map(one_block, (fields[step_number].reshape(-1, block_size, SLAB), current.reshape(-1, block_size, NORB, NEL), living.reshape(-1, block_size)))
        current = jnp.take(propagated.reshape(slot_count, NORB, NEL), sources[step_number], axis=0)
    return current
```

```python
import functools

import jax
import jax.numpy as jnp
from jax import lax
from jax.experimental import pallas as pl
from jax.experimental.pallas import tpu as pltpu
from jax.sharding import PartitionSpec as P

MESH = pl.DeviceIdType.MESH
ORDER = 4
VMEM_BYTES = 60 * 1024 * 1024


def taylor_step(potential, initial):
    summed = initial.astype(jnp.float32)
    term_now = initial
    for degree in range(1, ORDER + 1):
        product = jnp.dot(potential, term_now, preferred_element_type=jnp.float32) / degree
        summed = summed + product
        term_now = product.astype(jnp.bfloat16)
    return summed.astype(jnp.bfloat16)


def thin_rows(walkers, cholesky, slab_index, fields, counts, sources):
    steps, slab = slab_index.shape
    local_rows = walkers.shape[1]
    orbitals = cholesky.shape[2]
    per_device = fields.shape[1]
    row_devices = lax.axis_size("row")
    slot_count = per_device * row_devices
    my_index = lax.axis_index("row")
    all_fields = lax.all_gather(fields, "row", axis=1, tiled=True)
    slot_ids = jnp.arange(slot_count, dtype=jnp.int32)
    owners = slot_ids // per_device
    within = slot_ids % per_device
    owner_counts = jnp.take(counts, owners)
    living = within < owner_counts
    before = jnp.cumsum(counts) - counts
    live_total = jnp.sum(counts)
    owner_before = jnp.take(before, owners)
    ordinal = jnp.where(
        living,
        owner_before + within,
        live_total + owners * per_device - owner_before + within - owner_counts,
    )
    position = ordinal % row_devices * per_device + ordinal // row_devices
    placed = jnp.zeros((slot_count,), jnp.int32).at[position].set(slot_ids)
    busy_slots = (live_total - my_index + row_devices - 1) // row_devices
    current = walkers
    for step_number in range(steps):
        chosen = jnp.take(cholesky, slab_index[step_number], axis=0).reshape(
            slab, local_rows * orbitals
        )
        ordered_fields = jnp.take(all_fields[step_number], placed, axis=0)
        potential_rows = (
            jnp.dot(ordered_fields, chosen, preferred_element_type=jnp.float32)
            .astype(jnp.bfloat16)
            .reshape(slot_count, local_rows, orbitals)
        )
        ordered = jnp.take(current, placed, axis=0)
        potentials, columns = (
            lax.all_to_all(potential_rows, "row", split_axis=0, concat_axis=1, tiled=True),
            lax.all_to_all(ordered, "row", split_axis=0, concat_axis=1, tiled=True),
        )

        def advance(walker, buffer):
            matrix = lax.dynamic_index_in_dim(potentials, walker, 0, keepdims=False)
            initial = lax.dynamic_index_in_dim(columns, walker, 0, keepdims=False)
            return lax.dynamic_update_index_in_dim(buffer, taylor_step(matrix, initial), walker, 0)

        advanced = lax.fori_loop(0, busy_slots, advance, jnp.zeros_like(columns))
        returned = lax.all_to_all(advanced, "row", split_axis=1, concat_axis=0, tiled=True)
        current = jnp.take(returned, jnp.take(position, sources[step_number]), axis=0)
    return current


def enter(n, groups, me, group, across):
    barrier = pltpu.get_barrier_semaphore()

    def greet(k, carry):
        pl.semaphore_signal(
            barrier, inc=1, device_id={"row": lax.rem(me + k, n)}, device_id_type=MESH
        )
        return carry

    lax.fori_loop(1, n, greet, 0)
    others = 0
    if across:
        for k in range(1, groups):
            others += 1
            pl.semaphore_signal(
                barrier,
                inc=1,
                device_id={"groups": lax.rem(group + k, groups)},
                device_id_type=MESH,
            )
    pl.semaphore_wait(barrier, n - 1 + others)


def gather_kernel(
    n, groups, fields, counts, sources, all_fields, all_counts, all_sources,
    landed, send, recv, far_send, far_recv,
):
    me, group = lax.axis_index("row"), lax.axis_index("groups")
    enter(n, groups, me, group, True)

    def copy(k, owner):
        return pltpu.make_async_remote_copy(
            src_ref=fields,
            dst_ref=landed.at[owner],
            send_sem=send.at[k],
            recv_sem=recv.at[k],
            device_id={"row": lax.rem(me + k, n)},
            device_id_type=MESH,
        )

    def far(which, k, owner):
        return pltpu.make_async_remote_copy(
            src_ref=(counts, sources)[which],
            dst_ref=(all_counts, all_sources)[which].at[owner],
            send_sem=far_send.at[which, k],
            recv_sem=far_recv.at[which, k],
            device_id={"groups": lax.rem(group + k, groups)},
            device_id_type=MESH,
        )

    def begin(k, carry):
        copy(k, me).start()
        return carry

    def finish(k, carry):
        copy(k, lax.rem(me - k + n, n)).wait()
        return carry

    lax.fori_loop(1, n, begin, 0)
    for k in range(1, groups):
        for which in range(2):
            far(which, k, group).start()
    landed[me] = fields[...]
    all_counts[group] = counts[...]
    all_sources[group] = sources[...]
    lax.fori_loop(1, n, finish, 0)
    for k in range(1, groups):
        for which in range(2):
            far(which, k, lax.rem(group - k + groups, groups)).wait()
    all_fields[...] = landed[...].astype(jnp.float32)


def gather_fields(n, groups, fields, counts, sources):
    steps, per, slab = fields.shape
    slots = n * per
    vmem = pl.BlockSpec(memory_space=pltpu.VMEM)
    return pl.pallas_call(
        functools.partial(gather_kernel, n, groups),
        out_shape=(
            jax.ShapeDtypeStruct((n, steps, per, slab), jnp.float32),
            jax.ShapeDtypeStruct((groups, 1, n), jnp.int32),
            jax.ShapeDtypeStruct((groups, steps, slots), jnp.int32),
        ),
        in_specs=[vmem] * 3,
        out_specs=(vmem,) * 3,
        scratch_shapes=[
            pltpu.VMEM((n, steps, per, slab), jnp.bfloat16),
            pltpu.SemaphoreType.DMA((n,)),
            pltpu.SemaphoreType.DMA((n,)),
            pltpu.SemaphoreType.DMA((2, groups)),
            pltpu.SemaphoreType.DMA((2, groups)),
        ],
        compiler_params=pltpu.CompilerParams(collective_id=0, has_side_effects=True),
        name="gather_fields",
    )(fields, counts.reshape(1, n), sources)


def potential_kernel(
    n, groups, per, block,
    slab_index, counts, sources, fields, walkers, cholesky,
    potential, ordered, parents, picks, fits,
    chosen, made, left, spread, need, rank, slot, chol_sem, walk_sem, out_sem,
):
    steps, slab = slab_index.shape
    slots = n * per
    rows, orbitals = chosen.shape[2], chosen.shape[3]
    group = lax.axis_index("groups")

    def slab_copy(s, g):
        return pltpu.make_async_copy(
            cholesky.at[slab_index[s, g]], chosen.at[s, g], chol_sem.at[s, g]
        )

    for s in range(steps):
        def fetch(g, carry):
            slab_copy(s, g).start()
            return carry

        lax.fori_loop(0, slab, fetch, 0)

    def plan(which):
        def clear(j, carry):
            for s in range(steps + 1):
                need[s, j] = 0
            for s in range(steps):
                slot[s, j] = 0
            return carry

        def live(j, carry):
            need[steps, j] = (lax.rem(j, per) < counts[which, 0, j // per]).astype(jnp.int32)
            return carry

        lax.fori_loop(0, slots, clear, 0)
        lax.fori_loop(0, slots, live, 0)
        total = 0
        for s in reversed(range(steps)):
            def mark(j, carry):
                @pl.when(need[s + 1, j] == 1)
                def _():
                    need[s, sources[which, s, j]] = 1

                return carry

            def number(j, count):
                rank[s, j] = count

                @pl.when(need[s, j] == 1)
                def _():
                    slot[s, count] = j

                return count + need[s, j]

            lax.fori_loop(0, slots, mark, 0)
            count = lax.fori_loop(0, slots, number, jnp.int32(0))
            total = jnp.maximum(total, count)
        return total

    largest = jnp.int32(0)
    for k in range(1, groups + 1):
        own = plan(lax.rem(group + k, groups))
        largest = jnp.maximum(largest, own)
    fits[0] = (largest <= n).astype(jnp.int32)

    def walker_copy(p):
        return pltpu.make_async_copy(walkers.at[slot[0, p]], ordered.at[p], walk_sem.at[p])

    def take_walker(p, carry):
        walker_copy(p).start()
        return carry

    lax.fori_loop(0, slots, take_walker, 0)

    def parent(p, carry):
        for s in range(1, steps):
            index = slot[s, p]
            known = need[s, index]
            parents[s - 1, p] = known * (1 + rank[s - 1, sources[group, s - 1, index]])
        alive = need[steps, p]
        picks[p] = alive * (1 + rank[steps - 1, sources[group, steps - 1, p]])
        return carry

    lax.fori_loop(0, slots, parent, 0)

    wide = slab * block
    column = lax.broadcasted_iota(jnp.int32, (slab, wide), 1)
    owner = lax.broadcasted_iota(jnp.int32, (slab, wide), 0)
    expand = jnp.where(column // block == owner, 1.0, 0.0).astype(jnp.bfloat16)

    def out_copy(s, q):
        return pltpu.make_async_copy(made.at[s], potential.at[s, pl.ds(q * n, n)], out_sem.at[s])

    def build(s, q):
        def field_row(p, carry):
            index = slot[s, q * n + p]
            line = fields[index // per, s, pl.ds(lax.rem(index, per), 1), :]
            spread[pl.ds(pl.multiple_of(p * block, block), block), :] = jnp.broadcast_to(
                line, (block, slab)
            )
            return carry

        lax.fori_loop(0, n, field_row, 0)
        across = jnp.dot(
            spread[...].astype(jnp.bfloat16), expand, preferred_element_type=jnp.float32
        )
        row_in = lax.broadcasted_iota(jnp.int32, across.shape, 0) % block
        column_in = lax.broadcasted_iota(jnp.int32, across.shape, 1) % block
        left[...] = jnp.where(row_in == column_in, across, 0.0).astype(jnp.bfloat16)

        def tile(b, carry):
            lines = pl.ds(pl.multiple_of(b * block, block), block)
            width = min(256, orbitals)
            for c in range(0, orbitals, width):
                right = chosen[s, :, lines, c : c + width].reshape(wide, width)
                product = jnp.dot(left[...], right, preferred_element_type=jnp.float32)
                made[s, :, lines, c : c + width] = product.astype(jnp.bfloat16).reshape(
                    n, block, width
                )
            return carry

        lax.fori_loop(0, rows // block, tile, 0)
        out_copy(s, q).start()

    for s in range(steps):
        def arrive(g, carry):
            slab_copy(s, g).wait()
            return carry

        lax.fori_loop(0, slab, arrive, 0)
        build(s, 0)
    for s in range(steps):
        out_copy(s, 0).wait()

    for q in range(1, per):
        @pl.when(largest > n)
        def _():
            for s in range(steps):
                build(s, q)
            for s in range(steps):
                out_copy(s, q).wait()

    def walker_here(p, carry):
        walker_copy(p).wait()
        return carry

    lax.fori_loop(0, slots, walker_here, 0)


def make_potentials(n, groups, slab_index, counts, sources, fields, walkers, cholesky):
    _, steps, per, slab = fields.shape
    slots, rows, electrons = walkers.shape
    orbitals = cholesky.shape[2]
    block = 16
    smem = pl.BlockSpec(memory_space=pltpu.SMEM)
    vmem = pl.BlockSpec(memory_space=pltpu.VMEM)
    anywhere = pl.BlockSpec(memory_space=pl.ANY)
    return pl.pallas_call(
        functools.partial(potential_kernel, n, groups, per, block),
        out_shape=(
            jax.ShapeDtypeStruct((steps, slots, rows, orbitals), jnp.bfloat16),
            jax.ShapeDtypeStruct((slots, rows, electrons), jnp.bfloat16),
            jax.ShapeDtypeStruct((max(steps - 1, 1), slots), jnp.int32),
            jax.ShapeDtypeStruct((slots,), jnp.int32),
            jax.ShapeDtypeStruct((1,), jnp.int32),
        ),
        in_specs=[smem, smem, smem, vmem, anywhere, anywhere],
        out_specs=(anywhere, vmem, smem, smem, smem),
        scratch_shapes=[
            pltpu.VMEM((steps, slab, rows, orbitals), jnp.bfloat16),
            pltpu.VMEM((steps, n, rows, orbitals), jnp.bfloat16),
            pltpu.VMEM((n * block, slab * block), jnp.bfloat16),
            pltpu.VMEM((n * block, slab), jnp.float32),
            pltpu.SMEM((steps + 1, slots), jnp.int32),
            pltpu.SMEM((steps, slots), jnp.int32),
            pltpu.SMEM((steps, slots), jnp.int32),
            pltpu.SemaphoreType.DMA((steps, slab)),
            pltpu.SemaphoreType.DMA((slots,)),
            pltpu.SemaphoreType.DMA((steps,)),
        ],
        compiler_params=pltpu.CompilerParams(vmem_limit_bytes=VMEM_BYTES),
        name="make_potentials",
    )(slab_index, counts, sources, fields, walkers, cholesky)


def propagate_kernel(
    n, per, potential, ordered, parents, picks, out,
    matrices, columns, term, summed, advanced, turned, back0, back1,
    v_send, v_recv, w_send, w_recv, r_send, r_recv, own_sem,
):
    steps = potential.shape[0]
    rows, orbitals = potential.shape[2], potential.shape[3]
    electrons = ordered.shape[2]
    me = lax.axis_index("row")
    back = (back0, back1)

    def copy(source, target, sends, recvs, k):
        return pltpu.make_async_remote_copy(
            src_ref=source,
            dst_ref=target,
            send_sem=sends,
            recv_sem=recvs,
            device_id={"row": lax.rem(me + k, n)},
            device_id_type=MESH,
        )

    def v_copy(s, q, k, owner):
        return copy(
            potential.at[s, q * n + lax.rem(me + k, n)],
            matrices.at[s, q, owner],
            v_send.at[s, q, k],
            v_recv.at[s, q, k],
            k,
        )

    def w_copy(s, q, k, owner):
        source = ordered if s == 0 else turned
        return copy(
            source.at[q * n + lax.rem(me + k, n)],
            columns.at[s, q, owner],
            w_send.at[s, q, k],
            w_recv.at[s, q, k],
            k,
        )

    def r_copy(s, q, k, owner):
        return copy(
            advanced.at[s, q, lax.rem(me + k, n)],
            back[s].at[1 + q * n + owner],
            r_send.at[s, q, k],
            r_recv.at[s, q, k],
            k,
        )

    def own_v(s, q):
        return pltpu.make_async_copy(
            potential.at[s, q * n + me], matrices.at[s, q, me], own_sem.at[s, q]
        )

    def own_w(q):
        return pltpu.make_async_copy(
            ordered.at[q * n + me], columns.at[0, q, me], own_sem.at[steps, q]
        )

    def start(make, s, first=1, last=n):
        def one(k, carry):
            for q in range(per):
                make(s, q, k, me).start()
            return carry

        lax.fori_loop(first, last, one, 0)

    def received(make, s):
        def one(k, carry):
            for q in range(per):
                make(s, q, k, lax.rem(me - k + n, n)).wait_recv()
            return carry

        lax.fori_loop(1, n, one, 0)

    def sent(make, s):
        def one(k, carry):
            for q in range(per):
                make(s, q, k, me).wait_send()
            return carry

        lax.fori_loop(1, n, one, 0)

    def taylor(s, q):
        term[0] = columns[s, q].reshape(n * rows, electrons)
        summed[...] = columns[s, q].reshape(n * rows, electrons).astype(jnp.float32)
        height = max(rows, min(256, n * rows))
        count = height // rows

        def degree(k, carry):
            now, later = lax.rem(k - 1, 2), lax.rem(k, 2)
            scale = jnp.where(k == 1, 1.0, jnp.where(k == 2, 0.5, jnp.where(k == 3, 1 / 3, 0.25)))
            scale = scale.astype(jnp.float32)
            for c in range(n // count):
                matrix = matrices[s, q, c * count : (c + 1) * count].reshape(height, orbitals)
                product = (
                    jnp.dot(matrix, term[now], preferred_element_type=jnp.float32) * scale
                )
                lines = slice(c * height, (c + 1) * height)
                summed[lines, :] = summed[lines, :] + product
                term[later, lines, :] = product.astype(jnp.bfloat16)
            return carry

        lax.fori_loop(1, ORDER + 1, degree, 0)
        advanced[s, q] = summed[...].astype(jnp.bfloat16).reshape(n, rows, electrons)

    for s in range(steps):
        back[s][0] = jnp.zeros((rows, electrons), jnp.bfloat16)
    enter(n, 1, me, 0, False)
    start(w_copy, 0)
    start(v_copy, 0)
    for q in range(per):
        own_w(q).start()
        for s in range(steps):
            own_v(s, q).start()
    for q in range(per):
        own_w(q).wait()
        for s in range(steps):
            own_v(s, q).wait()
    received(w_copy, 0)
    received(v_copy, 0)
    for s in range(steps):
        if s + 1 < steps:
            start(v_copy, s + 1, 1, n // 2)
        for q in range(per):
            taylor(s, q)
        start(r_copy, s)
        if s + 1 < steps:
            start(v_copy, s + 1, n // 2, n)
        for q in range(per):
            back[s][1 + q * n + me] = advanced[s, q, me]
        received(r_copy, s)
        if s + 1 < steps:
            def turn(p, carry):
                turned[p] = back[s][parents[s, p]]
                return carry

            lax.fori_loop(0, n * per, turn, 0)
            start(w_copy, s + 1)
            for q in range(per):
                columns[s + 1, q, me] = turned[q * n + me]
            received(w_copy, s + 1)
            received(v_copy, s + 1)

    def pick(j, carry):
        out[j] = back[steps - 1][picks[j]]
        return carry

    lax.fori_loop(0, out.shape[0], pick, 0)
    for s in range(steps):
        for make in (w_copy, v_copy, r_copy):
            sent(make, s)


def propagate(n, per, ident, potential, ordered, parents, picks):
    steps, slots, rows, orbitals = potential.shape
    electrons = ordered.shape[2]
    smem = pl.BlockSpec(memory_space=pltpu.SMEM)
    anywhere = pl.BlockSpec(memory_space=pl.ANY)
    vmem = pl.BlockSpec(memory_space=pltpu.VMEM)
    half = jnp.bfloat16
    pairs = pltpu.SemaphoreType.DMA((steps, per, n))
    return pl.pallas_call(
        functools.partial(propagate_kernel, n, per),
        out_shape=jax.ShapeDtypeStruct((slots, rows, electrons), half),
        in_specs=[anywhere, anywhere, smem, smem],
        out_specs=vmem,
        scratch_shapes=[
            pltpu.VMEM((steps, per, n, rows, orbitals), half),
            pltpu.VMEM((steps, per, n, rows, electrons), half),
            pltpu.VMEM((2, n * rows, electrons), half),
            pltpu.VMEM((n * rows, electrons), jnp.float32),
            pltpu.VMEM((steps, per, n, rows, electrons), half),
            pltpu.VMEM((per * n, rows, electrons), half),
            pltpu.VMEM((1 + per * n, rows, electrons), half),
            pltpu.VMEM((1 + per * n, rows, electrons), half),
            pairs, pairs, pairs, pairs, pairs, pairs,
            pltpu.SemaphoreType.DMA((steps + 1, per)),
        ],
        compiler_params=pltpu.CompilerParams(
            collective_id=ident, has_side_effects=True, vmem_limit_bytes=VMEM_BYTES
        ),
        name="propagate_%d" % per,
    )(potential, ordered, parents, picks)


def on_device(n, groups, walkers, cholesky, slab_index, fields, counts, sources):
    if walkers.shape[1] % 16:
        return thin_rows(walkers, cholesky, slab_index, fields, counts, sources)
    per = fields.shape[1]
    all_fields, all_counts, all_sources = gather_fields(n, groups, fields, counts, sources)
    potential, ordered, parents, picks, fits = make_potentials(
        n, groups, slab_index, all_counts, all_sources, all_fields, walkers, cholesky
    )
    return lax.cond(
        fits[0] == 1,
        lambda *args: propagate(n, 1, 1, *args),
        lambda *args: propagate(n, per, 2, *args),
        potential, ordered, parents, picks,
    )


def solution(mesh):
    in_specs = (
        P("groups", "row", None),
        P("groups", "row", None),
        P("groups", None),
        P(None, ("groups", "row"), None),
        P("groups"),
        P("groups", None),
    )
    out_specs = P("groups", "row", None)
    return jax.shard_map(
        functools.partial(on_device, mesh.shape["row"], mesh.shape["groups"]),
        mesh=mesh, in_specs=in_specs, out_specs=out_specs, check_vma=False,
    )
```

```python
import functools

import jax
import jax.numpy as jnp
from jax import lax
from jax.experimental import pallas as pl
from jax.experimental.pallas import tpu as pltpu
from jax.sharding import PartitionSpec as P

MESH = pl.DeviceIdType.MESH
ORDER = 4
VMEM_BYTES = 60 * 1024 * 1024


def taylor_step(potential, initial):
    summed = initial.astype(jnp.float32)
    term_now = initial
    for degree in range(1, ORDER + 1):
        product = jnp.dot(potential, term_now, preferred_element_type=jnp.float32) / degree
        summed = summed + product
        term_now = product.astype(jnp.bfloat16)
    return summed.astype(jnp.bfloat16)


def thin_rows(walkers, cholesky, slab_index, fields, counts, sources):
    steps, slab = slab_index.shape
    local_rows = walkers.shape[1]
    orbitals = cholesky.shape[2]
    per_device = fields.shape[1]
    row_devices = lax.axis_size("row")
    slot_count = per_device * row_devices
    my_index = lax.axis_index("row")
    all_fields = lax.all_gather(fields, "row", axis=1, tiled=True)
    slot_ids = jnp.arange(slot_count, dtype=jnp.int32)
    owners = slot_ids // per_device
    within = slot_ids % per_device
    owner_counts = jnp.take(counts, owners)
    living = within < owner_counts
    before = jnp.cumsum(counts) - counts
    live_total = jnp.sum(counts)
    owner_before = jnp.take(before, owners)
    ordinal = jnp.where(
        living,
        owner_before + within,
        live_total + owners * per_device - owner_before + within - owner_counts,
    )
    position = ordinal % row_devices * per_device + ordinal // row_devices
    placed = jnp.zeros((slot_count,), jnp.int32).at[position].set(slot_ids)
    busy_slots = (live_total - my_index + row_devices - 1) // row_devices
    current = walkers
    for step_number in range(steps):
        chosen = jnp.take(cholesky, slab_index[step_number], axis=0).reshape(
            slab, local_rows * orbitals
        )
        ordered_fields = jnp.take(all_fields[step_number], placed, axis=0)
        potential_rows = (
            jnp.dot(ordered_fields, chosen, preferred_element_type=jnp.float32)
            .astype(jnp.bfloat16)
            .reshape(slot_count, local_rows, orbitals)
        )
        ordered = jnp.take(current, placed, axis=0)
        potentials, columns = (
            lax.all_to_all(potential_rows, "row", split_axis=0, concat_axis=1, tiled=True),
            lax.all_to_all(ordered, "row", split_axis=0, concat_axis=1, tiled=True),
        )

        def advance(walker, buffer):
            matrix = lax.dynamic_index_in_dim(potentials, walker, 0, keepdims=False)
            initial = lax.dynamic_index_in_dim(columns, walker, 0, keepdims=False)
            return lax.dynamic_update_index_in_dim(buffer, taylor_step(matrix, initial), walker, 0)

        advanced = lax.fori_loop(0, busy_slots, advance, jnp.zeros_like(columns))
        returned = lax.all_to_all(advanced, "row", split_axis=1, concat_axis=0, tiled=True)
        current = jnp.take(returned, jnp.take(position, sources[step_number]), axis=0)
    return current


def enter(n, groups, me, group, across):
    barrier = pltpu.get_barrier_semaphore()

    def greet(k, carry):
        pl.semaphore_signal(
            barrier, inc=1, device_id={"row": lax.rem(me + k, n)}, device_id_type=MESH
        )
        return carry

    lax.fori_loop(1, n, greet, 0)
    others = 0
    if across:
        for k in range(1, groups):
            others += 1
            pl.semaphore_signal(
                barrier,
                inc=1,
                device_id={"groups": lax.rem(group + k, groups)},
                device_id_type=MESH,
            )
    pl.semaphore_wait(barrier, n - 1 + others)


def gather_kernel(
    n, groups, fields, counts, sources, all_fields, all_counts, all_sources,
    landed, send, recv, far_send, far_recv,
):
    me, group = lax.axis_index("row"), lax.axis_index("groups")
    enter(n, groups, me, group, True)

    def copy(k, owner):
        return pltpu.make_async_remote_copy(
            src_ref=fields,
            dst_ref=landed.at[owner],
            send_sem=send.at[k],
            recv_sem=recv.at[k],
            device_id={"row": lax.rem(me + k, n)},
            device_id_type=MESH,
        )

    def far(which, k, owner):
        return pltpu.make_async_remote_copy(
            src_ref=(counts, sources)[which],
            dst_ref=(all_counts, all_sources)[which].at[owner],
            send_sem=far_send.at[which, k],
            recv_sem=far_recv.at[which, k],
            device_id={"groups": lax.rem(group + k, groups)},
            device_id_type=MESH,
        )

    def begin(k, carry):
        copy(k, me).start()
        return carry

    def finish(k, carry):
        copy(k, lax.rem(me - k + n, n)).wait()
        return carry

    lax.fori_loop(1, n, begin, 0)
    for k in range(1, groups):
        for which in range(2):
            far(which, k, group).start()
    landed[me] = fields[...]
    all_counts[group] = counts[...]
    all_sources[group] = sources[...]
    lax.fori_loop(1, n, finish, 0)
    for k in range(1, groups):
        for which in range(2):
            far(which, k, lax.rem(group - k + groups, groups)).wait()
    all_fields[...] = landed[...].astype(jnp.float32)


def gather_fields(n, groups, fields, counts, sources):
    steps, per, slab = fields.shape
    slots = n * per
    vmem = pl.BlockSpec(memory_space=pltpu.VMEM)
    return pl.pallas_call(
        functools.partial(gather_kernel, n, groups),
        out_shape=(
            jax.ShapeDtypeStruct((n, steps, per, slab), jnp.float32),
            jax.ShapeDtypeStruct((groups, 1, n), jnp.int32),
            jax.ShapeDtypeStruct((groups, steps, slots), jnp.int32),
        ),
        in_specs=[vmem] * 3,
        out_specs=(vmem,) * 3,
        scratch_shapes=[
            pltpu.VMEM((n, steps, per, slab), jnp.bfloat16),
            pltpu.SemaphoreType.DMA((n,)),
            pltpu.SemaphoreType.DMA((n,)),
            pltpu.SemaphoreType.DMA((2, groups)),
            pltpu.SemaphoreType.DMA((2, groups)),
        ],
        compiler_params=pltpu.CompilerParams(collective_id=0, has_side_effects=True),
        name="gather_fields",
    )(fields, counts.reshape(1, n), sources)


def room(n, share):
    return sum(share[plane % 2] for plane in range(n // 4)) if share else n


def seat(share, device):
    if share is None:
        return 1, device
    plane, place = lax.div(device, 4), lax.rem(device, 4)
    odd = lax.rem(plane, 2)
    idle = 1 + 2 * lax.rem(lax.div(plane, 2) + plane, 2)
    apart = place - idle

    def of(taken):
        if taken == 4:
            return 1, place
        if taken == 3:
            return 1 - lax.div(9 - apart * apart, 9), place - lax.div(place + 3 - idle, 4)
        return 1 - lax.rem(place, 2), lax.div(place, 2)

    (even_busy, even_place), (odd_busy, odd_place) = of(share[0]), of(share[1])
    first = lax.div(plane, 2) * (share[0] + share[1]) + odd * share[0]
    busy = (1 - odd) * even_busy + odd * odd_busy
    return busy, first + (1 - odd) * even_place + odd * odd_place


def potential_kernel(
    n, groups, per, block, shares,
    slab_index, counts, sources, fields, walkers, cholesky,
    potential, ordered, parents, picks, fits,
    chosen, made, left, spread, need, rank, slot, chol_sem, walk_sem, out_sem,
):
    steps, slab = slab_index.shape
    slots = n * per
    rows, orbitals = chosen.shape[2], chosen.shape[3]
    group = lax.axis_index("groups")
    unroll = slots <= 64

    def slab_copy(s, g):
        return pltpu.make_async_copy(
            cholesky.at[slab_index[s, g]], chosen.at[s, g], chol_sem.at[s, g]
        )

    for s in range(steps):
        def fetch(g, carry):
            slab_copy(s, g).start()
            return carry

        lax.fori_loop(0, slab, fetch, 0)

    def plan(which):
        def clear(j, carry):
            for s in range(steps + 1):
                need[s, j] = 0
            for s in range(steps):
                slot[s, j] = 0
            return carry

        def live(j, carry):
            need[steps, j] = (lax.rem(j, per) < counts[which, 0, lax.div(j, per)]).astype(jnp.int32)
            return carry

        lax.fori_loop(0, slots, clear, 0, unroll=unroll)
        lax.fori_loop(0, slots, live, 0, unroll=unroll)
        totals = [None] * steps
        for s in reversed(range(steps)):
            def mark(j, carry):
                picked = sources[which, s, j]
                need[s, picked] = jnp.maximum(need[s, picked], need[s + 1, j])
                return carry

            def number(j, count):
                rank[s, j] = count
                slot[s, count] = j
                return count + need[s, j]

            lax.fori_loop(0, slots, mark, 0, unroll=unroll)
            totals[s] = lax.fori_loop(0, slots, number, jnp.int32(0), unroll=unroll)
        return totals

    most = [jnp.int32(0)] * steps
    for k in range(1, groups + 1):
        own = plan(lax.rem(group + k, groups))
        most = [jnp.maximum(a, b) for a, b in zip(most, own)]
    largest = functools.reduce(jnp.maximum, most)
    choice = jnp.int32(len(shares))
    for place, share in reversed(list(enumerate(shares))):
        enough = most[0] <= room(n, share[0])
        for s in range(1, steps):
            enough = jnp.logical_and(enough, most[s] <= room(n, share[s]))
        choice = jnp.where(enough, place, choice)
    fits[0] = choice

    def walker_copy(p):
        return pltpu.make_async_copy(walkers.at[slot[0, p]], ordered.at[p], walk_sem.at[p])

    def take_walker(p, carry):
        walker_copy(p).start()
        return carry

    lax.fori_loop(0, slots, take_walker, 0)

    def parent(p, carry):
        for s in range(1, steps):
            index = slot[s, p]
            known = need[s, index]
            parents[s - 1, p] = known * (1 + rank[s - 1, sources[group, s - 1, index]])
        alive = need[steps, p]
        picks[p] = alive * (1 + rank[steps - 1, sources[group, steps - 1, p]])
        return carry

    lax.fori_loop(0, slots, parent, 0, unroll=unroll)

    wide = slab * block
    column = lax.broadcasted_iota(jnp.int32, (slab, wide), 1)
    owner = lax.broadcasted_iota(jnp.int32, (slab, wide), 0)
    expand = jnp.where(column // block == owner, 1.0, 0.0).astype(jnp.bfloat16)

    def out_copy(s, q):
        return pltpu.make_async_copy(made.at[s], potential.at[s, pl.ds(q * n, n)], out_sem.at[s])

    def build(s, q):
        def field_row(p, carry):
            index = slot[s, q * n + p]
            line = fields[lax.div(index, per), s, pl.ds(lax.rem(index, per), 1), :]
            spread[pl.ds(pl.multiple_of(p * block, block), block), :] = jnp.broadcast_to(
                line, (block, slab)
            )
            return carry

        lax.fori_loop(0, n, field_row, 0, unroll=unroll)
        across = jnp.dot(
            spread[...].astype(jnp.bfloat16), expand, preferred_element_type=jnp.float32
        )
        row_in = lax.broadcasted_iota(jnp.int32, across.shape, 0) % block
        column_in = lax.broadcasted_iota(jnp.int32, across.shape, 1) % block
        left[...] = jnp.where(row_in == column_in, across, 0.0).astype(jnp.bfloat16)

        def tile(b, carry):
            lines = pl.ds(pl.multiple_of(b * block, block), block)
            width = min(256, orbitals)
            for c in range(0, orbitals, width):
                right = chosen[s, :, lines, c : c + width].reshape(wide, width)
                product = jnp.dot(left[...], right, preferred_element_type=jnp.float32)
                made[s, :, lines, c : c + width] = product.astype(jnp.bfloat16).reshape(
                    n, block, width
                )
            return carry

        lax.fori_loop(0, rows // block, tile, 0)
        out_copy(s, q).start()

    for s in range(steps):
        def arrive(g, carry):
            slab_copy(s, g).wait()
            return carry

        lax.fori_loop(0, slab, arrive, 0)
        build(s, 0)
    for s in range(steps):
        out_copy(s, 0).wait()

    for q in range(1, per):
        @pl.when(largest > n)
        def _():
            for s in range(steps):
                build(s, q)
            for s in range(steps):
                out_copy(s, q).wait()

    def walker_here(p, carry):
        walker_copy(p).wait()
        return carry

    lax.fori_loop(0, slots, walker_here, 0)


def make_potentials(n, groups, shares, slab_index, counts, sources, fields, walkers, cholesky):
    _, steps, per, slab = fields.shape
    slots, rows, electrons = walkers.shape
    orbitals = cholesky.shape[2]
    block = 16
    smem = pl.BlockSpec(memory_space=pltpu.SMEM)
    vmem = pl.BlockSpec(memory_space=pltpu.VMEM)
    anywhere = pl.BlockSpec(memory_space=pl.ANY)
    return pl.pallas_call(
        functools.partial(potential_kernel, n, groups, per, block, shares),
        out_shape=(
            jax.ShapeDtypeStruct((steps, slots, rows, orbitals), jnp.bfloat16),
            jax.ShapeDtypeStruct((slots, rows, electrons), jnp.bfloat16),
            jax.ShapeDtypeStruct((max(steps - 1, 1), slots), jnp.int32),
            jax.ShapeDtypeStruct((slots,), jnp.int32),
            jax.ShapeDtypeStruct((1,), jnp.int32),
        ),
        in_specs=[smem, smem, smem, vmem, anywhere, anywhere],
        out_specs=(anywhere, vmem, smem, smem, smem),
        scratch_shapes=[
            pltpu.VMEM((steps, slab, rows, orbitals), jnp.bfloat16),
            pltpu.VMEM((steps, n, rows, orbitals), jnp.bfloat16),
            pltpu.VMEM((n * block, slab * block), jnp.bfloat16),
            pltpu.VMEM((n * block, slab), jnp.float32),
            pltpu.SMEM((steps + 1, slots), jnp.int32),
            pltpu.SMEM((steps, slots), jnp.int32),
            pltpu.SMEM((steps, slots), jnp.int32),
            pltpu.SemaphoreType.DMA((steps, slab)),
            pltpu.SemaphoreType.DMA((slots,)),
            pltpu.SemaphoreType.DMA((steps,)),
        ],
        compiler_params=pltpu.CompilerParams(vmem_limit_bytes=VMEM_BYTES),
        name="make_potentials",
    )(slab_index, counts, sources, fields, walkers, cholesky)


def propagate_kernel(
    n, per, share, potential, ordered, parents, picks, out,
    matrices, columns, term, summed, advanced, turned, back0, back1,
    v_send, v_recv, w_send, w_recv, r_send, r_recv, own_sem,
):
    steps = potential.shape[0]
    rows, orbitals = potential.shape[2], potential.shape[3]
    electrons = ordered.shape[2]
    me = lax.axis_index("row")
    back = (back0, back1)
    place = [seat(share[s], me)[1] for s in range(steps)]

    def copy(source, target, sends, recvs, k):
        return pltpu.make_async_remote_copy(
            src_ref=source,
            dst_ref=target,
            send_sem=sends,
            recv_sem=recvs,
            device_id={"row": lax.rem(me + k, n)},
            device_id_type=MESH,
        )

    def v_copy(s, q, k, owner):
        return copy(
            potential.at[s, q * n + seat(share[s], lax.rem(me + k, n))[1]],
            matrices.at[s, q, owner],
            v_send.at[s, q, k],
            v_recv.at[s, q, k],
            k,
        )

    def w_copy(s, q, k, owner):
        source = ordered if s == 0 else turned
        return copy(
            source.at[q * n + seat(share[s], lax.rem(me + k, n))[1]],
            columns.at[s, q, owner],
            w_send.at[s, q, k],
            w_recv.at[s, q, k],
            k,
        )

    def r_copy(s, q, k, owner):
        return copy(
            advanced.at[s, q, lax.rem(me + k, n)],
            back[s].at[1 + q * n + seat(share[s], owner)[1]],
            r_send.at[s, q, k],
            r_recv.at[s, q, k],
            k,
        )

    def own_v(s, q):
        return pltpu.make_async_copy(
            potential.at[s, q * n + place[s]], matrices.at[s, q, me], own_sem.at[s, q]
        )

    def own_w(q):
        return pltpu.make_async_copy(
            ordered.at[q * n + place[0]], columns.at[0, q, me], own_sem.at[steps, q]
        )

    def when(s, device):
        return pl.when(seat(share[s], device)[0] == 1) if share[s] else lambda body: body()

    def over(s, owned, turn, first=1, last=n):
        def one(k, carry):
            other = lax.rem(me + owned * k + n, n)

            @when(s, other if owned else me)
            def _():
                for q in range(per):
                    turn(q, k)

            return carry

        lax.fori_loop(first, last, one, 0)

    def start(make, s, first=1, last=n):
        over(s, 0 if make is r_copy else 1, lambda q, k: make(s, q, k, me).start(), first, last)

    def received(make, s):
        over(
            s,
            -1 if make is r_copy else 0,
            lambda q, k: make(s, q, k, lax.rem(me - k + n, n)).wait_recv(),
        )

    def sent(make, s):
        over(s, 0 if make is r_copy else 1, lambda q, k: make(s, q, k, me).wait_send())

    def taylor(s, q):
        term[0] = columns[s, q].reshape(n * rows, electrons)
        summed[...] = columns[s, q].reshape(n * rows, electrons).astype(jnp.float32)
        height = max(rows, min(256, n * rows))
        count = height // rows

        def degree(k, carry):
            now, later = lax.rem(k - 1, 2), lax.rem(k, 2)
            scale = jnp.where(k == 1, 1.0, jnp.where(k == 2, 0.5, jnp.where(k == 3, 1 / 3, 0.25)))
            scale = scale.astype(jnp.float32)
            for c in range(n // count):
                matrix = matrices[s, q, c * count : (c + 1) * count].reshape(height, orbitals)
                product = (
                    jnp.dot(matrix, term[now], preferred_element_type=jnp.float32) * scale
                )
                lines = slice(c * height, (c + 1) * height)
                summed[lines, :] = summed[lines, :] + product
                term[later, lines, :] = product.astype(jnp.bfloat16)
            return carry

        lax.fori_loop(1, ORDER + 1, degree, 0)
        advanced[s, q] = summed[...].astype(jnp.bfloat16).reshape(n, rows, electrons)

    for s in range(steps):
        for p in [0] + list(range(1 + per * room(n, share[s]), 1 + per * n)):
            back[s][p] = jnp.zeros((rows, electrons), jnp.bfloat16)
    enter(n, 1, me, 0, False)
    start(w_copy, 0)
    start(v_copy, 0)
    @when(0, me)
    def _():
        for q in range(per):
            own_w(q).start()
            own_v(0, q).start()

    for s in range(1, steps):
        @when(s, me)
        def _():
            for q in range(per):
                own_v(s, q).start()

    @when(0, me)
    def _():
        for q in range(per):
            own_w(q).wait()
            own_v(0, q).wait()

    for s in range(1, steps):
        @when(s, me)
        def _():
            for q in range(per):
                own_v(s, q).wait()

    received(w_copy, 0)
    received(v_copy, 0)
    for s in range(steps):
        if s + 1 < steps:
            start(v_copy, s + 1, 1, n // 2)

        @when(s, me)
        def _():
            for q in range(per):
                taylor(s, q)

        start(r_copy, s)
        if s + 1 < steps:
            start(v_copy, s + 1, n // 2, n)

        @when(s, me)
        def _():
            for q in range(per):
                back[s][1 + q * n + place[s]] = advanced[s, q, me]

        received(r_copy, s)
        if s + 1 < steps:
            def turn(p, carry):
                turned[p] = back[s][parents[s, p]]
                return carry

            lax.fori_loop(0, per * room(n, share[s + 1]), turn, 0)
            start(w_copy, s + 1)

            @when(s + 1, me)
            def _():
                for q in range(per):
                    columns[s + 1, q, me] = turned[q * n + place[s + 1]]

            received(w_copy, s + 1)
            received(v_copy, s + 1)

    def pick(j, carry):
        out[j] = back[steps - 1][picks[j]]
        return carry

    lax.fori_loop(0, out.shape[0], pick, 0)
    for s in range(steps):
        for make in (w_copy, v_copy, r_copy):
            sent(make, s)


def propagate(n, per, share, ident, potential, ordered, parents, picks):
    steps, slots, rows, orbitals = potential.shape
    electrons = ordered.shape[2]
    smem = pl.BlockSpec(memory_space=pltpu.SMEM)
    anywhere = pl.BlockSpec(memory_space=pl.ANY)
    vmem = pl.BlockSpec(memory_space=pltpu.VMEM)
    half = jnp.bfloat16
    pairs = pltpu.SemaphoreType.DMA((steps, per, n))
    return pl.pallas_call(
        functools.partial(propagate_kernel, n, per, share),
        out_shape=jax.ShapeDtypeStruct((slots, rows, electrons), half),
        in_specs=[anywhere, anywhere, smem, smem],
        out_specs=vmem,
        scratch_shapes=[
            pltpu.VMEM((steps, per, n, rows, orbitals), half),
            pltpu.VMEM((steps, per, n, rows, electrons), half),
            pltpu.VMEM((2, n * rows, electrons), half),
            pltpu.VMEM((n * rows, electrons), jnp.float32),
            pltpu.VMEM((steps, per, n, rows, electrons), half),
            pltpu.VMEM((per * n, rows, electrons), half),
            pltpu.VMEM((1 + per * n, rows, electrons), half),
            pltpu.VMEM((1 + per * n, rows, electrons), half),
            pairs, pairs, pairs, pairs, pairs, pairs,
            pltpu.SemaphoreType.DMA((steps + 1, per)),
        ],
        compiler_params=pltpu.CompilerParams(
            collective_id=ident, has_side_effects=True, vmem_limit_bytes=VMEM_BYTES
        ),
        name="propagate_%d" % ident,
    )(potential, ordered, parents, picks)


def on_device(n, groups, walkers, cholesky, slab_index, fields, counts, sources):
    if walkers.shape[1] % 16:
        return thin_rows(walkers, cholesky, slab_index, fields, counts, sources)
    steps, per = fields.shape[:2]
    shares = [(None,) * steps]
    if n % 4 == 0 and steps == 2:
        shares = [((3, 2), (3, 3)), ((3, 3), (4, 3))] + shares
    all_fields, all_counts, all_sources = gather_fields(n, groups, fields, counts, sources)
    potential, ordered, parents, picks, fits = make_potentials(
        n, groups, shares, slab_index, all_counts, all_sources, all_fields, walkers, cholesky
    )
    branches = [functools.partial(propagate, n, 1, share, 1 + i) for i, share in enumerate(shares)]
    branches.append(functools.partial(propagate, n, per, (None,) * steps, 1 + len(shares)))
    return lax.switch(fits[0], branches, potential, ordered, parents, picks)


def solution(mesh):
    in_specs = (
        P("groups", "row", None),
        P("groups", "row", None),
        P("groups", None),
        P(None, ("groups", "row"), None),
        P("groups"),
        P("groups", None),
    )
    out_specs = P("groups", "row", None)
    return jax.shard_map(
        functools.partial(on_device, mesh.shape["row"], mesh.shape["groups"]),
        mesh=mesh, in_specs=in_specs, out_specs=out_specs, check_vma=False,
    )
```
